256 devices in a mesh: rep: 64 (over y, z, core), shard: 4 (over x).
Axes of the slice: x: 4, y: 4, z: 8, core: 2. Of those that a mesh axis runs over, the one named last changes fastest.
Arguments:
- activ: bfloat16 [32768, 8192], P(('rep', 'shard')), may hold values from -6 to 6
- key_grad: bfloat16 [32768, 640], P(('rep', 'shard')), may hold values from -1.1953125 to 1.1953125
- key_weight: bfloat16 [8192, 640], P('shard'), may hold values from -0.25 to 0.25
- feedback: bfloat16 [64, 40960, 128], P('rep', 'shard'), may hold values from -24 to 24
- kept: int32 [64, 4, 512], P('rep', 'shard'), may hold values from 0 to 10239, as said below
- region_len: int32 [4, 64], P('shard'), may hold values from 80 to 240, as said below
Outputs:
- input_grad: bfloat16 [32768, 8192], P(('rep', 'shard'))
- next_feedback: bfloat16 [64, 40960, 128], P('rep', 'shard')
- owned_sum: float32 [4, 15360, 128], P('shard', 'rep')
The draws below stay inside these ranges and needn't reach their ends.
Inputs may be any that keep to these rules, and one draw needn't show every extreme that they name: `region_len`: each row splits its shard's 10240 blocks into 64 regions in order of owner and sums to 10240; every row has a region of exactly 240 blocks. `kept`: the 512 numbers of a row are different blocks of that shard. At most 16 of them lie in one region of the shard; every row has exactly 16 in some region, and in every shard some region gets exactly 16 from every replica.
All inputs are finite; a program needn't handle non-finite values.
Results may differ from the reference program's by a relative error of at most 0.011.
Values may be sent and summed in bfloat16 or wider, within the bound.
No kernel may reach another device: no remote copies, remote signals or barrier semaphores. Data moves between devices by JAX's collectives and lax.ppermute only.
A program may use at most 128 MiB of HBM per device.

```python
import jax
import jax.numpy as jnp
from jax import lax

D = 8192
BLK = 128
KEEP = 512
HK = 640
TOKENS = 32768
NBLK = 40960
NBS = 10240
REGION_MAX = 240
N_REP = 64
N_SHARD = 4


def paired(seed_key, center, spread, count, lead_owner):
    key_perm, key_step = jax.random.split(seed_key)
    serial = jax.random.permutation(key_perm, count).astype(jnp.int32)
    first_id = serial[0]
    serial = jnp.where(serial == lead_owner, first_id, serial)
    serial = serial.at[0].set(lead_owner)
    halves = count // 2
    spreads = jax.random.randint(key_step, (halves,), 0, spread + 1).astype(jnp.int32)
    spreads = spreads.at[0].set(spread)
    values = jnp.concatenate([center + spreads, center - spreads]).astype(jnp.int32)
    return jnp.zeros((count,), jnp.int32).at[serial].set(values)


def layout(seed_key):
    base_key = jax.random.fold_in(seed_key, 7301)
    block_count = NBLK // N_SHARD
    mean_len = block_count // N_REP
    shard_keys = jax.random.split(jax.random.fold_in(base_key, 1), N_SHARD)
    lead_len = jax.random.randint(jax.random.fold_in(base_key, 2), (N_SHARD,), 0, N_REP).astype(jnp.int32)

    def one_shard(shard_key, lead_owner):
        return paired(shard_key, mean_len, mean_len // 2, N_REP, lead_owner)
    lengths = jax.vmap(one_shard)(shard_keys, lead_len)
    starts = (jnp.cumsum(lengths, axis=1) - lengths).astype(jnp.int32)
    lead_take = jax.random.randint(jax.random.fold_in(base_key, 3), (N_SHARD,), 0, N_REP).astype(jnp.int32)
    per_owner = KEEP // N_REP
    row_keys = jax.random.split(jax.random.fold_in(base_key, 4), N_REP * N_SHARD)
    shard_of = jnp.arange(N_REP * N_SHARD, dtype=jnp.int32) % N_SHARD

    def pick(row_key, shard):
        key_first, key_second, key_third = jax.random.split(row_key, 3)
        counts = paired(key_first, per_owner, per_owner, N_REP, lead_take[shard])
        start_row = starts[shard]
        blocks = jnp.arange(block_count, dtype=jnp.int32)
        region = (jnp.searchsorted(start_row, blocks, side='right') - 1).astype(jnp.int32)
        noise = jax.random.permutation(key_second, block_count).astype(jnp.int32)
        serial = jnp.argsort(region * block_count + noise, stable=True).astype(jnp.int32)
        region_sorted = region[serial]
        region_rank = jnp.arange(block_count, dtype=jnp.int32) - start_row[region_sorted]
        keep_flags = region_rank < counts[region_sorted]
        picked = jnp.argsort(jnp.where(keep_flags, 0, 1).astype(jnp.int32), stable=True)[:KEEP]
        chosen = serial[picked]
        return chosen[jax.random.permutation(key_third, KEEP)].astype(jnp.int32)
    kept = jax.vmap(pick)(row_keys, shard_of).reshape(N_REP, N_SHARD, KEEP)
    return (lengths, kept)


def draw_region_len(key, part):
    return layout(key)[0]


def draw_kept(key, part):
    return layout(key)[1]


def block_scale(key, dims, cuts, smallest, high):
    gain, own = 1.0, jax.random.fold_in(key, 6)
    for position, parts in cuts:
        heights = jnp.exp(jax.random.uniform(jax.random.fold_in(own, position), (parts,), jnp.float32, smallest / len(cuts), high / len(cuts)))
        gain = gain * jnp.repeat(heights, dims[position] // parts).reshape([-1 if axis == position else 1 for axis in range(len(dims))])
    return gain


def normal_values(stream_key, extent, scale, most, shards=(), kind=jnp.bfloat16):
    drawn = scale * jax.random.normal(stream_key, extent, jnp.float32)
    if shards:
        drawn = drawn * block_scale(stream_key, extent, shards, -0.22, 0.18)
    return jnp.clip(drawn, -most, most).astype(kind)


def setup_inputs(seed: int = 0) -> dict:
    splits = jax.random.split(jax.random.key(seed), 7)
    activ = normal_values(splits[0], (TOKENS, D), 1.0, 6.0, ((0, 256),))
    key_grad = normal_values(splits[1], (TOKENS, HK), 0.2, 1.1953125, ((0, 256),))
    key_weight = normal_values(splits[2], (D, HK), HK ** -0.5, 0.25, ((0, 4),))
    feedback = normal_values(splits[3], (N_REP, NBLK, BLK), 4.0, 24.0, ((0, 64), (1, 4)))
    kept = draw_kept(jax.random.fold_in(splits[6], 71), 0)
    region_len = draw_region_len(jax.random.fold_in(splits[6], 71), 0)
    return {"activ": activ, "key_grad": key_grad, "key_weight": key_weight, "feedback": feedback, "kept": kept, "region_len": region_len}


def reference(activ, key_grad, key_weight, feedback, kept, region_len):
    input_grad = jnp.dot(key_grad, key_weight.T, preferred_element_type=jnp.float32).astype(jnp.bfloat16)
    rep_rows = TOKENS // N_REP
    act_rep = activ.reshape(N_REP, rep_rows, D)
    grad_rep = key_grad.reshape(N_REP, rep_rows, HK)
    shard_base = (jnp.arange(N_SHARD, dtype=jnp.int32) * NBS)[:, None]

    def renew(bundle):
        act_one, grad_one, fed_one, kept_one = bundle
        weight_grad = jnp.dot(act_one.T, grad_one, preferred_element_type=jnp.float32)
        flat_ids = (kept_one + shard_base).reshape(-1).astype(jnp.int32)
        chosen = jnp.zeros((NBLK,), bool).at[flat_ids].set(True)
        cleared = jnp.where(chosen[:, None], jnp.float32(0.0), fed_one.astype(jnp.float32))
        return (cleared + weight_grad.reshape(NBLK, BLK)).astype(jnp.bfloat16)

    next_feedback = lax.map(renew, (act_rep, grad_rep, feedback, kept))

    def fetch(fed_one, kept_one):
        return fed_one[(kept_one + shard_base).reshape(-1).astype(jnp.int32)]

    kept_values = jax.vmap(fetch)(feedback, kept).reshape(N_REP, N_SHARD, KEEP, BLK).astype(jnp.float32)
    starts = (jnp.cumsum(region_len, axis=1) - region_len).astype(jnp.int32)

    def collect(bundle):
        values_one, kept_shard, start_row = bundle
        owner_id = jnp.sum((start_row[None, None, :] <= kept_shard[:, :, None]).astype(jnp.int32), axis=2).astype(jnp.int32) - 1
        place_at = (owner_id * REGION_MAX + kept_shard - start_row[owner_id]).astype(jnp.int32)
        blank = jnp.zeros((N_REP * REGION_MAX, BLK), jnp.float32)
        return blank.at[place_at.reshape(-1)].add(values_one.reshape(-1, BLK))

    owned_sum = lax.map(collect, (jnp.swapaxes(kept_values, 0, 1), jnp.swapaxes(kept, 0, 1), starts))
    return input_grad, next_feedback, owned_sum
```

```python
import jax
import jax.numpy as jnp
from jax import lax
from jax.experimental import pallas as pl
from jax.experimental.pallas import tpu as pltpu
from jax.sharding import PartitionSpec as P

BF = jnp.bfloat16
F32 = jnp.float32
VMEM = pltpu.VMEM
SMEM = pltpu.SMEM
SLOTS = 16
ROWS = 24
BUCKET = 64
GROUP = 8


def prep_kernel(me_ref, kept_ref, len_ref, table_ref, send_ref, clear_ref, wide, outbox, base, low, high, count):
    blocks = table_ref.shape[0]
    owners = send_ref.shape[0]
    chunk = 512

    def widen(i, carry):
        rows = pl.ds(pl.multiple_of(i * chunk, chunk), chunk)
        wide[rows, :] = table_ref[rows, :].astype(F32)
        return carry

    lax.fori_loop(0, blocks // chunk, widen, 0)
    outbox[...] = jnp.zeros_like(outbox)

    def reset(i, carry):
        count[i] = 0
        return carry

    lax.fori_loop(0, owners, reset, 0, unroll=8)

    def tabulate(b, carry):
        owner, first, last = carry
        step = last <= b * BUCKET
        owner = jnp.where(step, owner + 1, owner)
        first = jnp.where(step, last, first)
        last = jnp.where(step, last + len_ref[0, owner], last)
        base[b] = owner
        low[b] = first
        high[b] = last
        return owner, first, last

    lax.fori_loop(0, blocks // BUCKET, tabulate, (jnp.int32(0), jnp.int32(0), len_ref[0, 0]), unroll=4)

    lane = lax.broadcasted_iota(jnp.int32, (1, 128), 1)
    lane_base = lax.rem(me_ref[0], GROUP) * SLOTS
    blank = jnp.zeros((1, 128), F32)

    def move(k, carry):
        block = kept_ref[0, 0, k]
        bucket = lax.shift_right_logical(block, 6)
        split = high[bucket]
        after = block >= split
        owner = base[bucket] + after.astype(jnp.int32)
        offset = block - jnp.where(after, split, low[bucket])
        slot = count[owner]
        count[owner] = slot + 1
        row = owner * ROWS
        outbox[pl.ds(row + slot, 1), :] = wide[pl.ds(block, 1), :]
        wide[pl.ds(block, 1), :] = blank
        tag = pl.ds(row + SLOTS, 1)
        outbox[tag, :] = jnp.where(lane == lane_base + slot, (offset + 1).astype(F32), outbox[tag, :])
        return carry

    lax.fori_loop(0, kept_ref.shape[2], move, 0, unroll=8)

    def narrow(i, carry):
        rows = pl.ds(pl.multiple_of(i * chunk, chunk), chunk)
        clear_ref[rows, :] = wide[rows, :].astype(BF)
        return carry

    lax.fori_loop(0, blocks // chunk, narrow, 0)
    for o in range(owners):
        send_ref[o] = outbox[o * ROWS : (o + 1) * ROWS, :].astype(BF)


def prep(me, kept, lengths, table, owners):
    blocks, width = table.shape
    smem = pl.BlockSpec(memory_space=SMEM)
    vmem = pl.BlockSpec(memory_space=VMEM)
    return pl.pallas_call(
        prep_kernel,
        out_shape=(
            jax.ShapeDtypeStruct((owners, ROWS, width), BF),
            jax.ShapeDtypeStruct((blocks, width), BF),
        ),
        in_specs=[smem, smem, smem, vmem],
        out_specs=(vmem, vmem),
        scratch_shapes=[
            VMEM((blocks, width), F32),
            VMEM((owners * ROWS, width), F32),
            SMEM((blocks // BUCKET,), jnp.int32),
            SMEM((blocks // BUCKET,), jnp.int32),
            SMEM((blocks // BUCKET,), jnp.int32),
            SMEM((owners,), jnp.int32),
        ],
        compiler_params=pltpu.CompilerParams(vmem_limit_bytes=24 << 20),
        cost_estimate=pl.CostEstimate(flops=30_000_000, bytes_accessed=4 * blocks * width, transcendentals=0),
        name="prep",
    )(me, kept, lengths, table)


def owned_kernel(got_ref, out_ref):
    region_max = out_ref.shape[0]
    row_id = lax.broadcasted_iota(jnp.int32, (region_max, 128), 0).astype(F32) + 1.0
    total = jnp.zeros(out_ref.shape, F32)
    for g in range(got_ref.shape[0] // GROUP):
        part = got_ref[g * GROUP : (g + 1) * GROUP]
        tags = jnp.sum(part[:, SLOTS, :].astype(F32), axis=0, keepdims=True)
        pick = (row_id == tags).astype(F32).astype(BF)
        rows = part[:, :SLOTS, :].reshape(GROUP * SLOTS, 128)
        total += jnp.dot(pick, rows, preferred_element_type=F32)
    out_ref[...] = total


def owned(got, region_max):
    return pl.pallas_call(
        owned_kernel,
        out_shape=jax.ShapeDtypeStruct((region_max, got.shape[2]), F32),
        in_specs=[pl.BlockSpec(memory_space=VMEM)],
        out_specs=pl.BlockSpec(memory_space=VMEM),
        cost_estimate=pl.CostEstimate(flops=4_000_000, bytes_accessed=got.size * 2, transcendentals=0),
        name="owned",
    )(got)


def grad_kernel(my_ref, a0, a1, a2, a3, g0, g1, g2, g3, clear_ref, out_ref, spread):
    acts = jnp.concatenate([a0[...], a1[...], a2[...], a3[...]], axis=0)
    grads = jnp.concatenate([g0[...], g1[...], g2[...], g3[...]], axis=0)
    total = lax.dot_general(acts, grads, (((0,), (0,)), ((), ())), preferred_element_type=F32)
    tile, keys = total.shape
    per = keys // 128
    for j in range(per):
        spread[pl.ds(j, tile, stride=per), :] = total[:, j * 128 : (j + 1) * 128]
    out_ref[...] = (clear_ref[...].astype(F32) + spread[...]).astype(BF)


def grad_update(my, activ, pieces, grads, cleared):
    tile = 256
    tokens, features = pieces[0].shape
    keys = grads[0].shape[1]
    per = keys // 128
    steps = features // tile
    piece = pl.BlockSpec((tokens, tile), lambda t, my: (0, t))
    whole = pl.BlockSpec((tokens, keys), lambda t, my: (0, 0))
    rows = pl.BlockSpec((tile * per, 128), lambda t, my: (t, 0))
    return pl.pallas_call(
        grad_kernel,
        out_shape=jax.ShapeDtypeStruct(cleared.shape, BF),
        grid_spec=pltpu.PrefetchScalarGridSpec(
            num_scalar_prefetch=1,
            grid=(steps,),
            in_specs=[pl.BlockSpec((tokens, tile), lambda t, my: (0, my[0] * steps + t))]
            + [piece] * 3 + [whole] * 4 + [rows],
            out_specs=rows,
            scratch_shapes=[VMEM((tile * per, 128), F32)],
        ),
        compiler_params=pltpu.CompilerParams(vmem_limit_bytes=24 << 20),
        cost_estimate=pl.CostEstimate(
            flops=2 * 4 * tokens * features * keys, bytes_accessed=12 << 20, transcendentals=0
        ),
        name="grad_update",
    )(my, activ, *pieces, *grads, cleared)


def place_kernel(my_ref, p0, p1, p2, p3, out_ref, sems):
    width = p0.shape[1]
    copies = []
    for j, piece in enumerate((p0, p1, p2, p3)):
        column = lax.rem(my_ref[0] + 4 - j, 4) * width
        copy = pltpu.make_async_copy(
            piece, out_ref.at[:, pl.ds(pl.multiple_of(column, width), width)], sems.at[j]
        )
        copy.start()
        copies.append(copy)
    for copy in copies:
        copy.wait()


def place(my, pieces):
    tokens, width = pieces[0].shape
    return pl.pallas_call(
        place_kernel,
        out_shape=jax.ShapeDtypeStruct((tokens, 4 * width), BF),
        in_specs=[pl.BlockSpec(memory_space=SMEM)] + [pl.BlockSpec(memory_space=VMEM)] * 4,
        out_specs=pl.BlockSpec(memory_space=pl.ANY),
        scratch_shapes=[pltpu.SemaphoreType.DMA((4,))],
        compiler_params=pltpu.CompilerParams(vmem_limit_bytes=8 << 20),
        cost_estimate=pl.CostEstimate(flops=1_000_000, bytes_accessed=4 << 20, transcendentals=0),
        name="place",
    )(my, *pieces)


def shift(x, k, n=4):
    return lax.ppermute(x, "shard", [(i, (i + k) % n) for i in range(n)])


def nt_dot(a, b):
    return lax.dot_general(a, b, (((1,), (1,)), ((), ())), preferred_element_type=F32).astype(BF)


def per_device(activ, key_grad, key_weight, feedback, kept, region_len):
    shards = lax.axis_size("shard")
    my = lax.axis_index("shard")
    me = lax.axis_index("rep").reshape(1)
    my1 = my.reshape(1)
    owners = lax.axis_size("rep")
    width = activ.shape[1] // shards
    kgs = {k: shift(key_grad, k) for k in (1, 3, 2)}
    outgoing = {
        k: lax.dynamic_slice_in_dim(activ, lax.rem(my + k, shards) * width, width, axis=1) for k in (1, 3, 2)
    }
    acts = {k: shift(outgoing[k], k) for k in (1, 3, 2)}
    table = feedback[0]
    blocks = table.shape[0]
    mean_len = blocks // owners
    send, cleared = prep(me, kept, region_len, table, owners)
    got = lax.all_to_all(send, "rep", split_axis=0, concat_axis=0, tiled=True)
    own_part = nt_dot(key_grad, key_weight)
    back = {k: shift(nt_dot(kgs[k], key_weight), shards - k) for k in (1, 3, 2)}
    updated = grad_update(
        my1, activ, [acts[1], acts[2], acts[3]], [key_grad, kgs[1], kgs[2], kgs[3]], cleared
    )
    owned_rows = owned(got, mean_len + mean_len // 2)
    input_grad = place(my1, [own_part, back[3], back[2], back[1]])
    return (input_grad, updated[None], owned_rows[None])


def solution(mesh):
    return jax.shard_map(
        per_device,
        mesh=mesh,
        in_specs=(
            P(("rep", "shard"), None),
            P(("rep", "shard"), None),
            P("shard", None),
            P("rep", "shard", None),
            P("rep", "shard", None),
            P("shard", None),
        ),
        out_specs=(P(("rep", "shard"), None), P("rep", "shard", None), P("shard", "rep", None)),
        check_vma=False,
    )
```

```python
import jax
import jax.numpy as jnp
from jax import lax
from jax.experimental import pallas as pl
from jax.experimental.pallas import tpu as pltpu
from jax.sharding import PartitionSpec as P


BF = jnp.bfloat16
F32 = jnp.float32
VMEM = pltpu.VMEM
SMEM = pltpu.SMEM
SLOTS = 16
ROWS = 24
BUCKET = 64
GROUP = 8


def pack_kernel(my_ref, activ_ref, o1, o2, o3, sems):
    width = o1.shape[1]
    copies = []
    for k, out in ((1, o1), (3, o3), (2, o2)):
        column = lax.rem(my_ref[0] + k, 4) * width
        copy = pltpu.make_async_copy(
            activ_ref.at[:, pl.ds(pl.multiple_of(column, width), width)], out, sems.at[k - 1]
        )
        copy.start()
        copies.append(copy)
    for copy in copies:
        copy.wait()


def pack(my, activ, width):
    piece = jax.ShapeDtypeStruct((activ.shape[0], width), BF)
    return pl.pallas_call(
        pack_kernel,
        out_shape=(piece,) * 3,
        in_specs=[pl.BlockSpec(memory_space=SMEM), pl.BlockSpec(memory_space=pltpu.HBM)],
        out_specs=(pl.BlockSpec(memory_space=VMEM),) * 3,
        scratch_shapes=[pltpu.SemaphoreType.DMA((3,))],
        compiler_params=pltpu.CompilerParams(vmem_limit_bytes=59 << 20),
        cost_estimate=pl.CostEstimate(flops=1_000_000, bytes_accessed=4 << 20, transcendentals=0),
        name="pack",
    )(my, activ)


def prep_kernel(
    me_ref, kept_ref, len_ref, table_ref, send_ref, clear_ref, held, wide, outbox, base, low, high, count, sems
):
    blocks = held.shape[0]
    owners = send_ref.shape[0]
    parts = sems.shape[0]
    part = blocks // parts
    chunk = 256

    def span(p):
        return pl.ds(p * part, part)

    loads = [pltpu.make_async_copy(table_ref.at[span(p)], held.at[span(p)], sems.at[p]) for p in range(parts)]
    for load in loads:
        load.start()
    outbox[...] = jnp.zeros_like(outbox)

    def reset(i, carry):
        count[i] = 0
        return carry

    lax.fori_loop(0, owners, reset, 0, unroll=8)

    def tabulate(b, carry):
        owner, first, last = carry
        step = last <= b * BUCKET
        owner = jnp.where(step, owner + 1, owner)
        first = jnp.where(step, last, first)
        last = jnp.where(step, last + len_ref[0, owner], last)
        base[b] = owner
        low[b] = first
        high[b] = last
        return owner, first, last

    lax.fori_loop(0, blocks // BUCKET, tabulate, (jnp.int32(0), jnp.int32(0), len_ref[0, 0]), unroll=4)

    def widen(i, carry):
        rows = pl.ds(pl.multiple_of(i * chunk, chunk), chunk)
        wide[rows, :] = held[rows, :].astype(F32)
        return carry

    for p, load in enumerate(loads):
        load.wait()
        lax.fori_loop(p * part // chunk, (p + 1) * part // chunk, widen, 0)

    lane = lax.broadcasted_iota(jnp.int32, (1, 128), 1)
    lane_base = lax.rem(me_ref[0], GROUP) * SLOTS
    blank = jnp.zeros((1, 128), F32)

    def move(k, carry):
        block = kept_ref[0, 0, k]
        bucket = lax.shift_right_logical(block, 6)
        split = high[bucket]
        after = block >= split
        owner = base[bucket] + after.astype(jnp.int32)
        offset = block - jnp.where(after, split, low[bucket])
        slot = count[owner]
        count[owner] = slot + 1
        row = owner * ROWS
        outbox[pl.ds(row + slot, 1), :] = wide[pl.ds(block, 1), :]
        wide[pl.ds(block, 1), :] = blank
        tag = pl.ds(row + SLOTS, 1)
        outbox[tag, :] = jnp.where(lane == lane_base + slot, (offset + 1).astype(F32), outbox[tag, :])
        return carry

    lax.fori_loop(0, kept_ref.shape[2], move, 0, unroll=8)

    def narrow(i, carry):
        rows = pl.ds(pl.multiple_of(i * chunk, chunk), chunk)
        held[rows, :] = wide[rows, :].astype(BF)
        return carry

    stores = []
    for p in range(parts):
        lax.fori_loop(p * part // chunk, (p + 1) * part // chunk, narrow, 0)
        store = pltpu.make_async_copy(held.at[span(p)], clear_ref.at[span(p)], sems.at[p])
        store.start()
        stores.append(store)
    for o in range(owners):
        send_ref[o] = outbox[o * ROWS : (o + 1) * ROWS, :].astype(BF)
    for store in stores:
        store.wait()


def prep(me, kept, lengths, table, owners):
    blocks, width = table.shape
    smem = pl.BlockSpec(memory_space=SMEM)
    vmem = pl.BlockSpec(memory_space=VMEM)
    whole = pl.BlockSpec(memory_space=pltpu.HBM)
    return pl.pallas_call(
        prep_kernel,
        out_shape=(
            jax.ShapeDtypeStruct((owners, ROWS, width), BF),
            jax.ShapeDtypeStruct((blocks, width), BF),
        ),
        in_specs=[smem, smem, smem, whole],
        out_specs=(vmem, whole),
        scratch_shapes=[
            VMEM((blocks, width), BF),
            VMEM((blocks, width), F32),
            VMEM((owners * ROWS, width), F32),
            SMEM((blocks // BUCKET,), jnp.int32),
            SMEM((blocks // BUCKET,), jnp.int32),
            SMEM((blocks // BUCKET,), jnp.int32),
            SMEM((owners,), jnp.int32),
            pltpu.SemaphoreType.DMA((4,)),
        ],
        compiler_params=pltpu.CompilerParams(vmem_limit_bytes=58 << 20),
        cost_estimate=pl.CostEstimate(flops=30_000_000, bytes_accessed=4 * blocks * width, transcendentals=0),
        name="prep",
    )(me, kept, lengths, table)


def owned_kernel(got_ref, out_ref):
    region_max = out_ref.shape[0]
    row_id = lax.broadcasted_iota(jnp.int32, (region_max, 128), 0).astype(F32) + 1.0
    total = jnp.zeros(out_ref.shape, F32)
    for g in range(got_ref.shape[0] // GROUP):
        part = got_ref[g * GROUP : (g + 1) * GROUP]
        tags = jnp.sum(part[:, SLOTS, :].astype(F32), axis=0, keepdims=True)
        pick = (row_id == tags).astype(F32).astype(BF)
        rows = part[:, :SLOTS, :].reshape(GROUP * SLOTS, 128)
        total += jnp.dot(pick, rows, preferred_element_type=F32)
    out_ref[...] = total


def owned(got, region_max):
    return pl.pallas_call(
        owned_kernel,
        out_shape=jax.ShapeDtypeStruct((region_max, got.shape[2]), F32),
        in_specs=[pl.BlockSpec(memory_space=VMEM)],
        out_specs=pl.BlockSpec(memory_space=VMEM),
        compiler_params=pltpu.CompilerParams(vmem_limit_bytes=4 << 20),
        cost_estimate=pl.CostEstimate(flops=4_000_000, bytes_accessed=got.size * 2, transcendentals=0),
        name="owned",
    )(got)


def grad_kernel(my_ref, a0, a1, a2, a3, g0, g1, g2, g3, clear_ref, out_ref, spread):
    acts = jnp.concatenate([a0[...], a1[...], a2[...], a3[...]], axis=0)
    grads = jnp.concatenate([g0[...], g1[...], g2[...], g3[...]], axis=0)
    total = lax.dot_general(acts, grads, (((0,), (0,)), ((), ())), preferred_element_type=F32)
    tile, keys = total.shape
    per = keys // 128
    for j in range(per):
        spread[pl.ds(j, tile, stride=per), :] = total[:, j * 128 : (j + 1) * 128]
    out_ref[...] = (clear_ref[...].astype(F32) + spread[...]).astype(BF)


def grad_update(my, activ, pieces, grads, cleared):
    tile = 256
    tokens, features = pieces[0].shape
    keys = grads[0].shape[1]
    per = keys // 128
    steps = features // tile
    piece = pl.BlockSpec((tokens, tile), lambda t, my: (0, t))
    whole = pl.BlockSpec((tokens, keys), lambda t, my: (0, 0))
    rows = pl.BlockSpec((tile * per, 128), lambda t, my: (t, 0))
    return pl.pallas_call(
        grad_kernel,
        out_shape=jax.ShapeDtypeStruct(cleared.shape, BF),
        grid_spec=pltpu.PrefetchScalarGridSpec(
            num_scalar_prefetch=1,
            grid=(steps,),
            in_specs=[pl.BlockSpec((tokens, tile), lambda t, my: (0, my[0] * steps + t))]
            + [piece] * 3 + [whole] * 4 + [rows],
            out_specs=rows,
            scratch_shapes=[VMEM((tile * per, 128), F32)],
        ),
        compiler_params=pltpu.CompilerParams(vmem_limit_bytes=58 << 20),
        cost_estimate=pl.CostEstimate(
            flops=2 * 4 * tokens * features * keys, bytes_accessed=12 << 20, transcendentals=0
        ),
        name="grad_update",
    )(my, activ, *pieces, *grads, cleared)


def place_kernel(my_ref, p0, p1, p2, p3, out_ref, sems):
    width = p0.shape[1]
    copies = []
    for j, piece in enumerate((p0, p1, p2, p3)):
        column = lax.rem(my_ref[0] + 4 - j, 4) * width
        copy = pltpu.make_async_copy(
            piece, out_ref.at[:, pl.ds(pl.multiple_of(column, width), width)], sems.at[j]
        )
        copy.start()
        copies.append(copy)
    for copy in copies:
        copy.wait()


def place(my, pieces):
    tokens, width = pieces[0].shape
    return pl.pallas_call(
        place_kernel,
        out_shape=jax.ShapeDtypeStruct((tokens, 4 * width), BF),
        in_specs=[pl.BlockSpec(memory_space=SMEM)] + [pl.BlockSpec(memory_space=VMEM)] * 4,
        out_specs=pl.BlockSpec(memory_space=pl.ANY),
        scratch_shapes=[pltpu.SemaphoreType.DMA((4,))],
        compiler_params=pltpu.CompilerParams(vmem_limit_bytes=8 << 20),
        cost_estimate=pl.CostEstimate(flops=1_000_000, bytes_accessed=4 << 20, transcendentals=0),
        name="place",
    )(my, *pieces)


def shift(x, k, n=4):
    return lax.ppermute(x, "shard", [(i, (i + k) % n) for i in range(n)])


def nt_dot(a, b):
    return lax.dot_general(a, b, (((1,), (1,)), ((), ())), preferred_element_type=F32).astype(BF)


def after(x, *earlier):
    return lax.optimization_barrier((x, *earlier))[0]


def step(activ, key_grad, key_weight, feedback, kept, region_len):
    shards = lax.axis_size("shard")
    my = lax.axis_index("shard")
    me = lax.axis_index("rep").reshape(1)
    my1 = my.reshape(1)
    owners = lax.axis_size("rep")
    width = activ.shape[1] // shards
    order = (1, 3, 2)
    kgs, acts, parts, back = {}, {}, {}, {}
    for k in order:
        kgs[k] = shift(key_grad, k)
    outgoing = dict(zip((1, 2, 3), pack(my1, activ, width)))
    for k in order:
        acts[k] = shift(outgoing[k], k)
    table = feedback[0]
    blocks = table.shape[0]
    mean_len = blocks // owners
    send, cleared = prep(me, kept, region_len, table, owners)
    for k in order:
        parts[k] = nt_dot(kgs[k], key_weight)
        back[k] = shift(parts[k], shards - k)
    own_part = nt_dot(key_grad, key_weight)
    send = after(send, own_part)
    got = lax.all_to_all(send, "rep", split_axis=0, concat_axis=0, tiled=True)
    updated = grad_update(
        my1, activ, [acts[1], acts[2], acts[3]], [key_grad, kgs[1], kgs[2], kgs[3]], cleared
    )
    owned_rows = owned(got, mean_len + mean_len // 2)
    pieces = lax.optimization_barrier(([own_part, back[3], back[2], back[1]], owned_rows))[0]
    input_grad = place(my1, pieces)
    return (input_grad, updated[None], owned_rows[None])


def solution(mesh):
    return jax.shard_map(
        step,
        mesh=mesh,
        in_specs=(
            P(("rep", "shard"), None),
            P(("rep", "shard"), None),
            P("shard", None),
            P("rep", "shard", None),
            P("rep", "shard", None),
            P("shard", None),
        ),
        out_specs=(P(("rep", "shard"), None), P("rep", "shard", None), P("shard", "rep", None)),
        check_vma=False,
    )
```

```python
import jax
import jax.numpy as jnp
from jax import lax
from jax.experimental import pallas as pl
from jax.experimental.pallas import tpu as pltpu
from jax.sharding import PartitionSpec as P


BF = jnp.bfloat16
F32 = jnp.float32
VMEM = pltpu.VMEM
SMEM = pltpu.SMEM
SLOTS = 16
ROWS = 24
GROUP = 8
TILE = 1024
PACK_LIMIT = 59
PREP_LIMIT = 58
GRAD_LIMIT = 50
DOTS_LIMIT = 40
DOTS_TILE = 1024


def bundle_copies(my, k, activ_ref, grad_ref, out, sems):
    keys = grad_ref.shape[1]
    width = out.shape[1] - keys
    column = pl.multiple_of(lax.rem(my + k, 4) * width, width)
    return [
        pltpu.make_async_copy(activ_ref.at[:, pl.ds(column, width)], out.at[:, keys:], sems.at[0]),
        pltpu.make_async_copy(grad_ref, out.at[:, :keys], sems.at[1]),
    ]


def pack_kernel(my_ref, index_ref, activ_ref, weight_ref, o1, o3, cut, sems):
    piece = cut.shape[0]
    first = pl.multiple_of(index_ref[0] * piece, piece)
    width = o1.shape[1]
    copies = [pltpu.make_async_copy(weight_ref.at[pl.ds(first, piece)], cut, sems.at[0])]
    for k, out in ((1, o1), (3, o3)):
        column = pl.multiple_of(lax.rem(my_ref[0] + k, 4) * width, width)
        copies.append(pltpu.make_async_copy(activ_ref.at[:, pl.ds(column, width)], out, sems.at[(k + 1) // 2]))
    for copy in copies:
        copy.start()
    for copy in copies:
        copy.wait()


def pack(my, index, activ, key_weight, width, piece):
    bundle = jax.ShapeDtypeStruct((activ.shape[0], width), BF)
    hbm = pl.BlockSpec(memory_space=pltpu.HBM)
    smem = pl.BlockSpec(memory_space=SMEM)
    return pl.pallas_call(
        pack_kernel,
        out_shape=(bundle, bundle, jax.ShapeDtypeStruct((piece, key_weight.shape[1]), BF)),
        in_specs=[smem, smem, hbm, hbm],
        out_specs=(pl.BlockSpec(memory_space=VMEM),) * 3,
        scratch_shapes=[pltpu.SemaphoreType.DMA((3,))],
        compiler_params=pltpu.CompilerParams(vmem_limit_bytes=PACK_LIMIT << 20),
        cost_estimate=pl.CostEstimate(flops=1_000_000, bytes_accessed=3 << 20, transcendentals=0),
        name="pack",
    )(my, index, activ, key_weight)


def nt(a, b):
    return lax.dot_general(a, b, (((1,), (1,)), ((), ())), preferred_element_type=F32)


def iota(shape, dim):
    return lax.broadcasted_iota(jnp.int32, shape, dim)


def bits(mask):
    return mask.astype(F32).astype(BF)


def prep_kernel(
    me_ref, my_ref, kept_ref, ids_ref, len_ref, table_ref, activ_ref, grad_ref,
    send_ref, mask_ref, o2, held, wide, outbox, spot_v, spot_s, sems, spot_sem, pack_sems
):
    blocks = held.shape[0]
    owners = send_ref.shape[0]
    keep = ids_ref.shape[2]
    parts = sems.shape[0]
    part = blocks // parts
    chunk = 256

    def span(p):
        return pl.ds(p * part, part)

    loads = [pltpu.make_async_copy(table_ref.at[span(p)], held.at[span(p)], sems.at[p]) for p in range(parts)]
    for load in loads:
        load.start()
    packs = bundle_copies(my_ref[0], 2, activ_ref, grad_ref, o2, pack_sems)
    for copy in packs:
        copy.start()

    ids = ids_ref[0]
    lengths = len_ref[...]
    starts = jnp.sum(
        jnp.where(iota((owners, owners), 1) < iota((owners, owners), 0), lengths, 0), axis=1, keepdims=True
    )
    ends = jnp.sum(
        jnp.where(iota((owners, owners), 1) <= iota((owners, owners), 0), lengths, 0), axis=1, keepdims=True
    )
    inside = ((ids >= starts) & (ids < ends)).astype(F32)
    before = bits(iota((keep, keep), 1) > iota((keep, keep), 0))
    earlier = lax.dot_general(inside.astype(BF), before, (((1,), (0,)), ((), ())), preferred_element_type=F32)
    slot = jnp.sum(inside * earlier, axis=0, keepdims=True)
    owner = jnp.sum(inside * iota((owners, 1), 0).astype(F32), axis=0, keepdims=True)
    offset = ids.astype(F32) - jnp.sum(inside * starts.astype(F32), axis=0, keepdims=True)
    spot_v[...] = (owner * ROWS + slot).astype(jnp.int32)
    fetch = pltpu.make_async_copy(spot_v, spot_s, spot_sem)
    fetch.start()
    lane_base = lax.rem(me_ref[0], GROUP) * SLOTS
    lane = bits(iota((128, keep), 0) == slot.astype(jnp.int32) + lane_base)
    tags = nt((inside * (offset + 1.0)).astype(BF), lane)
    high = lax.shift_right_logical(ids, 7)
    low = bits(iota((128, keep), 0) == lax.bitwise_and(ids, 127))
    per = mask_ref.shape[0] // 128
    count = blocks // 128 // per
    for t in range(per):
        hit = bits(iota((128, keep), 0) == high - t * count)
        mask_ref[t * 128 : (t + 1) * 128, :] = nt(low, hit)
    outbox[...] = jnp.zeros_like(outbox)
    for o in range(owners):
        outbox[o * ROWS + SLOTS : o * ROWS + SLOTS + 1, :] = tags[o : o + 1, :]

    def widen(i, carry):
        rows = pl.ds(pl.multiple_of(i * chunk, chunk), chunk)
        wide[rows, :] = held[rows, :].astype(F32)
        return carry

    for p, load in enumerate(loads):
        load.wait()
        lax.fori_loop(p * part // chunk, (p + 1) * part // chunk, widen, 0)
    fetch.wait()

    def move(k, carry):
        outbox[pl.ds(spot_s[0, k], 1), :] = wide[pl.ds(kept_ref[0, 0, k], 1), :]
        return carry

    lax.fori_loop(0, keep, move, 0, unroll=16)
    for o in range(owners):
        send_ref[o] = outbox[o * ROWS : (o + 1) * ROWS, :].astype(BF)
    for copy in packs:
        copy.wait()


def prep(me, my, kept, lengths, table, activ, key_grad, owners, tiles):
    tokens, keys = key_grad.shape
    blocks, width = table.shape
    keep = kept.shape[2]
    smem = pl.BlockSpec(memory_space=SMEM)
    vmem = pl.BlockSpec(memory_space=VMEM)
    whole = pl.BlockSpec(memory_space=pltpu.HBM)
    return pl.pallas_call(
        prep_kernel,
        out_shape=(
            jax.ShapeDtypeStruct((owners, ROWS, width), BF),
            jax.ShapeDtypeStruct((tiles * 128, 128), F32),
            jax.ShapeDtypeStruct((tokens, keys + activ.shape[1] // 4), BF),
        ),
        in_specs=[smem, smem, smem, vmem, vmem, whole, whole, whole],
        out_specs=(vmem, vmem, vmem),
        scratch_shapes=[
            VMEM((blocks, width), BF),
            VMEM((blocks, width), F32),
            VMEM((owners * ROWS, width), F32),
            VMEM((1, keep), jnp.int32),
            SMEM((1, keep), jnp.int32),
            pltpu.SemaphoreType.DMA((4,)),
            pltpu.SemaphoreType.DMA,
            pltpu.SemaphoreType.DMA((2,)),
        ],
        compiler_params=pltpu.CompilerParams(vmem_limit_bytes=PREP_LIMIT << 20),
        cost_estimate=pl.CostEstimate(flops=30_000_000, bytes_accessed=4 * blocks * width, transcendentals=0),
        name="prep",
    )(me, my, kept, kept, lengths, table, activ, key_grad)


def owned_kernel(got_ref, out_ref):
    region_max = out_ref.shape[0]
    row_id = lax.broadcasted_iota(jnp.int32, (region_max, 128), 0).astype(F32) + 1.0
    total = jnp.zeros(out_ref.shape, F32)
    for g in range(got_ref.shape[0] // GROUP):
        part = got_ref[g * GROUP : (g + 1) * GROUP]
        tags = jnp.sum(part[:, SLOTS, :].astype(F32), axis=0, keepdims=True)
        pick = (row_id == tags).astype(F32).astype(BF)
        rows = part[:, :SLOTS, :].reshape(GROUP * SLOTS, 128)
        total += jnp.dot(pick, rows, preferred_element_type=F32)
    out_ref[...] = total


def owned(got, region_max):
    return pl.pallas_call(
        owned_kernel,
        out_shape=jax.ShapeDtypeStruct((region_max, got.shape[2]), F32),
        in_specs=[pl.BlockSpec(memory_space=VMEM)],
        out_specs=pl.BlockSpec(memory_space=VMEM),
        compiler_params=pltpu.CompilerParams(vmem_limit_bytes=4 << 20),
        cost_estimate=pl.CostEstimate(flops=4_000_000, bytes_accessed=got.size * 2, transcendentals=0),
        name="owned",
    )(got)


def grad_kernel(my_ref, a0, g0, b1, b2, b3, g1, g3, feed_ref, mask_ref, out_ref, spread, grads):
    tile = a0.shape[1]
    tokens, keys = g0.shape
    per = keys // 128
    step = pl.program_id(0)
    near = pl.ds(pl.multiple_of(step * tile, 128), tile)
    column = pl.ds(pl.multiple_of(keys + step * tile, 128), tile)

    @pl.when(step == 0)
    def _():
        grads[:tokens, :] = g0[...]
        grads[tokens : 2 * tokens, :] = g1[...]
        grads[2 * tokens : 3 * tokens, :] = b2[:, :keys]
        grads[3 * tokens :, :] = g3[...]

    acts = jnp.concatenate([a0[...], b1[:, near], b2[:, column], b3[:, near]], axis=0)
    total = lax.dot_general(acts, grads[...], (((0,), (0,)), ((), ())), preferred_element_type=F32)
    for j in range(per):
        spread[pl.ds(j, tile, stride=per), :] = total[:, j * 128 : (j + 1) * 128]
    mask = mask_ref[...]
    for i in range(tile * per // 128):
        rows = slice(i * 128, (i + 1) * 128)
        feed = feed_ref[rows, :].astype(F32)
        out_ref[rows, :] = (jnp.where(mask[:, i : i + 1] > 0.0, 0.0, feed) + spread[rows, :]).astype(BF)


def grad_update(my, activ, key_grad, bundles, near, table, mask):
    tile = TILE
    tokens, keys = key_grad.shape
    features = bundles[0].shape[1]
    per = keys // 128
    steps = features // tile
    vmem = pl.BlockSpec(memory_space=VMEM)
    rows = pl.BlockSpec((tile * per, 128), lambda t, my: (t, 0))
    return pl.pallas_call(
        grad_kernel,
        out_shape=jax.ShapeDtypeStruct(table.shape, BF),
        grid_spec=pltpu.PrefetchScalarGridSpec(
            num_scalar_prefetch=1,
            grid=(steps,),
            in_specs=[pl.BlockSpec((tokens, tile), lambda t, my: (0, my[0] * steps + t))]
            + [vmem] * 6 + [rows, pl.BlockSpec((128, 128), lambda t, my: (t, 0))],
            out_specs=rows,
            scratch_shapes=[VMEM((tile * per, 128), F32), VMEM((4 * tokens, keys), BF)],
        ),
        compiler_params=pltpu.CompilerParams(vmem_limit_bytes=GRAD_LIMIT << 20),
        cost_estimate=pl.CostEstimate(
            flops=2 * 4 * tokens * features * keys, bytes_accessed=12 << 20, transcendentals=0
        ),
        name="grad_update",
    )(my, activ, key_grad, *bundles, *near, table, mask)


def join_kernel(*refs):
    out_ref = refs[-1]
    rows = refs[0].shape[0]
    for i, ref in enumerate(refs[:-1]):
        out_ref[i * rows : (i + 1) * rows, :] = ref[...]


def join(pieces):
    rows, width = pieces[0].shape
    total = len(pieces) * rows
    return pl.pallas_call(
        join_kernel,
        out_shape=jax.ShapeDtypeStruct((total, width), BF),
        in_specs=[pl.BlockSpec(memory_space=VMEM)] * len(pieces),
        out_specs=pl.BlockSpec(memory_space=VMEM),
        compiler_params=pltpu.CompilerParams(vmem_limit_bytes=8 << 20),
        cost_estimate=pl.CostEstimate(flops=500_000, bytes_accessed=4 * total * width, transcendentals=0),
        name="join",
    )(*pieces)


def dots_kernel(my_ref, g0, b1, b3, weight_ref, p0, p1, p3):
    tokens = g0.shape[0]
    grads = jnp.concatenate([g0[...], b1[...], b3[...]], axis=0)
    product = nt(grads, weight_ref[...]).astype(BF)
    for i, out in enumerate((p0, p1, p3)):
        out[...] = product[i * tokens : (i + 1) * tokens, :]


def dots(my, key_grad, near, weight):
    tokens, keys = key_grad.shape
    features = weight.shape[0]
    tile = DOTS_TILE
    steps = features // tile
    grads = pl.BlockSpec((tokens, keys), lambda t, my: (0, 0))
    out = pl.BlockSpec((tokens, tile), lambda t, my: (0, t))
    return pl.pallas_call(
        dots_kernel,
        out_shape=(jax.ShapeDtypeStruct((tokens, 4 * features), BF),)
        + (jax.ShapeDtypeStruct((tokens, features), BF),) * 2,
        grid_spec=pltpu.PrefetchScalarGridSpec(
            num_scalar_prefetch=1,
            grid=(steps,),
            in_specs=[grads, grads, grads, pl.BlockSpec((tile, keys), lambda t, my: (t, 0))],
            out_specs=(pl.BlockSpec((tokens, tile), lambda t, my: (0, my[0] * steps + t)), out, out),
        ),
        compiler_params=pltpu.CompilerParams(vmem_limit_bytes=DOTS_LIMIT << 20),
        cost_estimate=pl.CostEstimate(
            flops=2 * 3 * tokens * features * keys, bytes_accessed=5 << 20, transcendentals=0
        ),
        name="dots",
    )(my, key_grad, near[0], near[1], weight)


def finish_kernel(my_ref, where_ref, grad_ref, near_ref, other_ref, p1, p3, begun_ref, out_ref, far, sems):
    half, _ = near_ref.shape
    width = p1.shape[1]
    y, z, core = where_ref[0], where_ref[1], where_ref[2]
    piece = half // 8

    def column(j):
        return pl.multiple_of(lax.rem(my_ref[0] + 4 - j, 4) * width, width)

    copies = []
    for j, ref in ((1, p1), (3, p3)):
        copy = pltpu.make_async_copy(ref, out_ref.at[:, pl.ds(column(j), width)], sems.at[j])
        copy.start()
        copies.append(copy)

    def fetch(ref, row, residue):
        turn_y = lax.rem(row + 4 - y, 4)
        turn_z = lax.rem(residue + z, 2)
        return ref[pl.ds(pl.multiple_of((turn_y * 2 + turn_z) * piece, piece), piece), :]

    grads = grad_ref[...]
    for source in range(2):
        ref = near_ref if source == 0 else other_ref
        side = core if source == 0 else 1 - core
        for row in range(4):
            rows = jnp.concatenate([fetch(ref, row, residue) for residue in range(2)], axis=0)
            at = pl.multiple_of(side * half + row * 2 * piece, 2 * piece)
            far[:, pl.ds(at, 2 * piece)] = nt(grads, rows).astype(BF)
    copy = pltpu.make_async_copy(far, out_ref.at[:, pl.ds(column(2), width)], sems.at[2])
    copy.start()
    copies.append(copy)
    for copy in copies:
        copy.wait()


def finish(my, where, key_grad, near, other, p1, p3, begun):
    tokens, width = p1.shape
    vmem = pl.BlockSpec(memory_space=VMEM)
    smem = pl.BlockSpec(memory_space=SMEM)
    return pl.pallas_call(
        finish_kernel,
        out_shape=jax.ShapeDtypeStruct((tokens, 4 * width), BF),
        in_specs=[smem, smem] + [vmem] * 5 + [pl.BlockSpec(memory_space=pltpu.HBM)],
        out_specs=pl.BlockSpec(memory_space=pltpu.HBM),
        input_output_aliases={7: 0},
        scratch_shapes=[VMEM((tokens, width), BF), pltpu.SemaphoreType.DMA((4,))],
        compiler_params=pltpu.CompilerParams(vmem_limit_bytes=16 << 20),
        cost_estimate=pl.CostEstimate(flops=300_000_000, bytes_accessed=6 << 20, transcendentals=0),
        name="finish",
    )(my, where, key_grad, near, other, p1, p3, begun)


def shift(x, k, n=4):
    return lax.ppermute(x, "shard", [(i, (i + k) % n) for i in range(n)])


def after(x, *earlier):
    return lax.optimization_barrier((x, *earlier))[0]


def turn(x, dy, dz, dc):
    pairs = []
    for y in range(4):
        for z in range(8):
            for c in range(2):
                to = (((y + dy) % 4) * 8 + (z ^ dz)) * 2 + (c ^ dc)
                pairs.append(((y * 8 + z) * 2 + c, to))
    return lax.ppermute(x, "rep", pairs)


def step(activ, key_grad, key_weight, feedback, kept, region_len):
    shards = lax.axis_size("shard")
    my = lax.axis_index("shard")
    rep = lax.axis_index("rep")
    me = rep.reshape(1)
    my1 = my.reshape(1)
    y, z, core = lax.div(rep, 16), lax.rem(lax.div(rep, 2), 8), lax.rem(rep, 2)
    where = jnp.stack([y, z, core])
    owners = lax.axis_size("rep")
    width = activ.shape[1] // shards
    piece = width // 16
    index = ((core * 4 + y) * 2 + lax.rem(z, 2)).reshape(1)
    grad_one = shift(key_grad, 1)
    grad_three = shift(key_grad, 3)
    one, three, mine = pack(my1, index, activ, key_weight, width, piece)
    mine = shift(mine, 2)
    bundle, back = {}, {}
    bundle[1] = shift(one, 1)
    bundle[3] = shift(three, 3)
    twin = turn(mine, 0, 1, 0)
    table = feedback[0]
    blocks = table.shape[0]
    mean_len = blocks // owners
    send, mask, two = prep(me, my1, kept, region_len, table, activ, key_grad, owners, width // TILE)
    bundle[2] = shift(two, 2)
    plane = join([mine, twin])
    grid = [plane, None, None, None]
    for dy in (1, 3, 2):
        grid[dy] = turn(plane, -dy, 0, 0)
    got = lax.all_to_all(send, "rep", split_axis=0, concat_axis=0, tiled=True)
    begun, *parts = dots(my1, key_grad, [grad_one, grad_three], key_weight)
    for k, part in zip((1, 3), parts):
        back[k] = shift(part, shards - k)
    near = join(grid)
    other = turn(near, 0, 0, 1)
    updated = grad_update(my1, activ, key_grad, [bundle[1], bundle[2], bundle[3]], [grad_one, grad_three], table, mask)
    owned_rows = owned(got, mean_len + mean_len // 2)
    last = after(back[1], owned_rows, updated)
    input_grad = finish(my1, where, key_grad, near, other, back[3], last, begun)
    return (input_grad, updated[None], owned_rows[None])


def solution(mesh):
    return jax.shard_map(
        step,
        mesh=mesh,
        in_specs=(
            P(("rep", "shard"), None),
            P(("rep", "shard"), None),
            P("shard", None),
            P("rep", "shard", None),
            P("rep", "shard", None),
            P("shard", None),
        ),
        out_specs=(P(("rep", "shard"), None), P("rep", "shard", None), P("shard", "rep", None)),
        check_vma=False,
    )
```

```python
import jax
import jax.numpy as jnp
from jax import lax
from jax.experimental import pallas as pl
from jax.experimental.pallas import tpu as pltpu
from jax.sharding import PartitionSpec as P


BF = jnp.bfloat16
F32 = jnp.float32
VMEM = pltpu.VMEM
SMEM = pltpu.SMEM
SLOTS = 16
ROWS = 24
GROUP = 8
TILE = 1024
PACK_LIMIT = 59
PREP_LIMIT = 58
GRAD_LIMIT = 53
DOTS_LIMIT = 40
DOTS_TILE = 1024
FINISH_LIMIT = 50


def bundle_copies(my, k, activ_ref, grad_ref, out, sems):
    keys = grad_ref.shape[1]
    width = out.shape[1] - keys
    column = pl.multiple_of(lax.rem(my + k, 4) * width, width)
    return [
        pltpu.make_async_copy(activ_ref.at[:, pl.ds(column, width)], out.at[:, keys:], sems.at[0]),
        pltpu.make_async_copy(grad_ref, out.at[:, :keys], sems.at[1]),
    ]


def pack_kernel(my_ref, index_ref, activ_ref, weight_ref, o1, o3, cut, sems):
    piece = cut.shape[0]
    first = pl.multiple_of(index_ref[0] * piece, piece)
    width = o1.shape[1]
    copies = [pltpu.make_async_copy(weight_ref.at[pl.ds(first, piece)], cut, sems.at[0])]
    for k, out in ((1, o1), (3, o3)):
        column = pl.multiple_of(lax.rem(my_ref[0] + k, 4) * width, width)
        copies.append(pltpu.make_async_copy(activ_ref.at[:, pl.ds(column, width)], out, sems.at[(k + 1) // 2]))
    for copy in copies:
        copy.start()
    for copy in copies:
        copy.wait()


def pack(my, index, activ, key_weight, width, piece):
    bundle = jax.ShapeDtypeStruct((activ.shape[0], width), BF)
    hbm = pl.BlockSpec(memory_space=pltpu.HBM)
    smem = pl.BlockSpec(memory_space=SMEM)
    return pl.pallas_call(
        pack_kernel,
        out_shape=(bundle, bundle, jax.ShapeDtypeStruct((piece, key_weight.shape[1]), BF)),
        in_specs=[smem, smem, hbm, hbm],
        out_specs=(pl.BlockSpec(memory_space=VMEM),) * 3,
        scratch_shapes=[pltpu.SemaphoreType.DMA((3,))],
        compiler_params=pltpu.CompilerParams(vmem_limit_bytes=PACK_LIMIT << 20),
        cost_estimate=pl.CostEstimate(flops=1_000_000, bytes_accessed=3 << 20, transcendentals=0),
        name="pack",
    )(my, index, activ, key_weight)


def nt(a, b):
    return lax.dot_general(a, b, (((1,), (1,)), ((), ())), preferred_element_type=F32)


def iota(shape, dim):
    return lax.broadcasted_iota(jnp.int32, shape, dim)


def bits(mask):
    return mask.astype(F32).astype(BF)


def prep_kernel(
    me_ref, my_ref, kept_ref, ids_ref, len_ref, table_ref, activ_ref, grad_ref,
    send_ref, o2, held, wide, outbox, spot_v, spot_s, sems, spot_sem, pack_sems
):
    blocks = held.shape[0]
    owners = send_ref.shape[0]
    keep = ids_ref.shape[2]
    parts = sems.shape[0]
    part = blocks // parts
    chunk = 256

    def span(p):
        return pl.ds(p * part, part)

    loads = [pltpu.make_async_copy(table_ref.at[span(p)], held.at[span(p)], sems.at[p]) for p in range(parts)]
    for load in loads:
        load.start()
    packs = bundle_copies(my_ref[0], 2, activ_ref, grad_ref, o2, pack_sems)
    for copy in packs:
        copy.start()

    ids = ids_ref[0]
    lengths = len_ref[...]
    starts = jnp.sum(
        jnp.where(iota((owners, owners), 1) < iota((owners, owners), 0), lengths, 0), axis=1, keepdims=True
    )
    ends = jnp.sum(
        jnp.where(iota((owners, owners), 1) <= iota((owners, owners), 0), lengths, 0), axis=1, keepdims=True
    )
    inside = ((ids >= starts) & (ids < ends)).astype(F32)
    before = bits(iota((keep, keep), 1) > iota((keep, keep), 0))
    earlier = lax.dot_general(inside.astype(BF), before, (((1,), (0,)), ((), ())), preferred_element_type=F32)
    slot = jnp.sum(inside * earlier, axis=0, keepdims=True)
    owner = jnp.sum(inside * iota((owners, 1), 0).astype(F32), axis=0, keepdims=True)
    offset = ids.astype(F32) - jnp.sum(inside * starts.astype(F32), axis=0, keepdims=True)
    spot_v[...] = (owner * ROWS + slot).astype(jnp.int32)
    fetch = pltpu.make_async_copy(spot_v, spot_s, spot_sem)
    fetch.start()
    lane_base = lax.rem(me_ref[0], GROUP) * SLOTS
    lane = bits(iota((128, keep), 0) == slot.astype(jnp.int32) + lane_base)
    tags = nt((inside * (offset + 1.0)).astype(BF), lane)
    outbox[...] = jnp.zeros_like(outbox)
    for o in range(owners):
        outbox[o * ROWS + SLOTS : o * ROWS + SLOTS + 1, :] = tags[o : o + 1, :]

    def widen(i, carry):
        rows = pl.ds(pl.multiple_of(i * chunk, chunk), chunk)
        wide[rows, :] = held[rows, :].astype(F32)
        return carry

    for p, load in enumerate(loads):
        load.wait()
        lax.fori_loop(p * part // chunk, (p + 1) * part // chunk, widen, 0)
    fetch.wait()

    def move(k, carry):
        outbox[pl.ds(spot_s[0, k], 1), :] = wide[pl.ds(kept_ref[0, 0, k], 1), :]
        return carry

    lax.fori_loop(0, keep, move, 0, unroll=16)
    for o in range(owners):
        send_ref[o] = outbox[o * ROWS : (o + 1) * ROWS, :].astype(BF)
    for copy in packs:
        copy.wait()


def prep(me, my, kept, lengths, table, activ, key_grad, owners):
    tokens, keys = key_grad.shape
    blocks, width = table.shape
    keep = kept.shape[2]
    smem = pl.BlockSpec(memory_space=SMEM)
    vmem = pl.BlockSpec(memory_space=VMEM)
    whole = pl.BlockSpec(memory_space=pltpu.HBM)
    return pl.pallas_call(
        prep_kernel,
        out_shape=(
            jax.ShapeDtypeStruct((owners, ROWS, width), BF),
            jax.ShapeDtypeStruct((tokens, keys + activ.shape[1] // 4), BF),
        ),
        in_specs=[smem, smem, smem, vmem, vmem, whole, whole, whole],
        out_specs=(vmem, vmem),
        scratch_shapes=[
            VMEM((blocks, width), BF),
            VMEM((blocks, width), F32),
            VMEM((owners * ROWS, width), F32),
            VMEM((1, keep), jnp.int32),
            SMEM((1, keep), jnp.int32),
            pltpu.SemaphoreType.DMA((4,)),
            pltpu.SemaphoreType.DMA,
            pltpu.SemaphoreType.DMA((2,)),
        ],
        compiler_params=pltpu.CompilerParams(vmem_limit_bytes=PREP_LIMIT << 20),
        cost_estimate=pl.CostEstimate(flops=30_000_000, bytes_accessed=4 * blocks * width, transcendentals=0),
        name="prep",
    )(me, my, kept, kept, lengths, table, activ, key_grad)


def owned_kernel(got_ref, out_ref):
    region_max = out_ref.shape[0]
    row_id = lax.broadcasted_iota(jnp.int32, (region_max, 128), 0).astype(F32) + 1.0
    total = jnp.zeros(out_ref.shape, F32)
    for g in range(got_ref.shape[0] // GROUP):
        part = got_ref[g * GROUP : (g + 1) * GROUP]
        tags = jnp.sum(part[:, SLOTS, :].astype(F32), axis=0, keepdims=True)
        pick = (row_id == tags).astype(F32).astype(BF)
        rows = part[:, :SLOTS, :].reshape(GROUP * SLOTS, 128)
        total += jnp.dot(pick, rows, preferred_element_type=F32)
    out_ref[...] = total


def owned(got, region_max):
    return pl.pallas_call(
        owned_kernel,
        out_shape=jax.ShapeDtypeStruct((region_max, got.shape[2]), F32),
        in_specs=[pl.BlockSpec(memory_space=VMEM)],
        out_specs=pl.BlockSpec(memory_space=VMEM),
        compiler_params=pltpu.CompilerParams(vmem_limit_bytes=4 << 20),
        cost_estimate=pl.CostEstimate(flops=4_000_000, bytes_accessed=got.size * 2, transcendentals=0),
        name="owned",
    )(got)


def grad_kernel(my_ref, a0, g0, b1, b2, b3, g1, g3, feed_ref, ids_ref, out_ref, spread, grads):
    tile = a0.shape[1]
    tokens, keys = g0.shape
    per = keys // 128
    step = pl.program_id(0)
    near = pl.ds(pl.multiple_of(step * tile, 128), tile)
    column = pl.ds(pl.multiple_of(keys + step * tile, 128), tile)

    @pl.when(step == 0)
    def _():
        grads[:tokens, :] = g0[...]
        grads[tokens : 2 * tokens, :] = g1[...]
        grads[2 * tokens : 3 * tokens, :] = b2[:, :keys]
        grads[3 * tokens :, :] = g3[...]

    acts = jnp.concatenate([a0[...], b1[:, near], b2[:, column], b3[:, near]], axis=0)
    total = lax.dot_general(acts, grads[...], (((0,), (0,)), ((), ())), preferred_element_type=F32)
    for j in range(per):
        spread[pl.ds(j, tile, stride=per), :] = total[:, j * 128 : (j + 1) * 128]
    ids = ids_ref[0]
    keep = ids.shape[1]
    count = tile * per // 128
    low = bits(iota((128, keep), 0) == lax.bitwise_and(ids, 127))
    hit = bits(iota((128, keep), 0) == lax.shift_right_logical(ids, 7) - step * count)
    mask = nt(low, hit)
    for i in range(tile * per // 128):
        rows = slice(i * 128, (i + 1) * 128)
        feed = feed_ref[rows, :].astype(F32)
        out_ref[rows, :] = (jnp.where(mask[:, i : i + 1] > 0.0, 0.0, feed) + spread[rows, :]).astype(BF)


def grad_update(my, activ, key_grad, bundles, near, table, kept):
    tile = TILE
    tokens, keys = key_grad.shape
    features = bundles[0].shape[1]
    per = keys // 128
    steps = features // tile
    vmem = pl.BlockSpec(memory_space=VMEM)
    rows = pl.BlockSpec((tile * per, 128), lambda t, my: (t, 0))
    return pl.pallas_call(
        grad_kernel,
        out_shape=jax.ShapeDtypeStruct(table.shape, BF),
        grid_spec=pltpu.PrefetchScalarGridSpec(
            num_scalar_prefetch=1,
            grid=(steps,),
            in_specs=[pl.BlockSpec((tokens, tile), lambda t, my: (0, my[0] * steps + t))]
            + [vmem] * 6 + [rows, vmem],
            out_specs=rows,
            scratch_shapes=[
                VMEM((tile * per, 128), F32),
                VMEM((4 * tokens, keys), BF),
            ],
        ),
        compiler_params=pltpu.CompilerParams(vmem_limit_bytes=GRAD_LIMIT << 20),
        cost_estimate=pl.CostEstimate(
            flops=2 * 4 * tokens * features * keys, bytes_accessed=12 << 20, transcendentals=0
        ),
        name="grad_update",
    )(my, activ, key_grad, *bundles, *near, table, kept)


def join_kernel(*refs):
    out_ref = refs[-1]
    rows = refs[0].shape[0]
    for i, ref in enumerate(refs[:-1]):
        out_ref[i * rows : (i + 1) * rows, :] = ref[...]


def join(pieces):
    rows, width = pieces[0].shape
    total = len(pieces) * rows
    return pl.pallas_call(
        join_kernel,
        out_shape=jax.ShapeDtypeStruct((total, width), BF),
        in_specs=[pl.BlockSpec(memory_space=VMEM)] * len(pieces),
        out_specs=pl.BlockSpec(memory_space=VMEM),
        compiler_params=pltpu.CompilerParams(vmem_limit_bytes=8 << 20),
        cost_estimate=pl.CostEstimate(flops=500_000, bytes_accessed=4 * total * width, transcendentals=0),
        name="join",
    )(*pieces)


def dots_kernel(my_ref, g0, b1, b3, weight_ref, p0, p1, p3):
    tokens = g0.shape[0]
    grads = jnp.concatenate([g0[...], b1[...], b3[...]], axis=0)
    product = nt(grads, weight_ref[...]).astype(BF)
    for i, out in enumerate((p0, p1, p3)):
        out[...] = product[i * tokens : (i + 1) * tokens, :]


def dots(my, key_grad, near, weight):
    tokens, keys = key_grad.shape
    features = weight.shape[0]
    tile = DOTS_TILE
    steps = features // tile
    grads = pl.BlockSpec((tokens, keys), lambda t, my: (0, 0))
    out = pl.BlockSpec((tokens, tile), lambda t, my: (0, t))
    return pl.pallas_call(
        dots_kernel,
        out_shape=(jax.ShapeDtypeStruct((tokens, 4 * features), BF),)
        + (jax.ShapeDtypeStruct((tokens, features), BF),) * 2,
        grid_spec=pltpu.PrefetchScalarGridSpec(
            num_scalar_prefetch=1,
            grid=(steps,),
            in_specs=[grads, grads, grads, pl.BlockSpec((tile, keys), lambda t, my: (t, 0))],
            out_specs=(pl.BlockSpec((tokens, tile), lambda t, my: (0, my[0] * steps + t)), out, out),
        ),
        compiler_params=pltpu.CompilerParams(vmem_limit_bytes=DOTS_LIMIT << 20),
        cost_estimate=pl.CostEstimate(
            flops=2 * 3 * tokens * features * keys, bytes_accessed=5 << 20, transcendentals=0
        ),
        name="dots",
    )(my, key_grad, near[0], near[1], weight)


def half_product(where_ref, grads, weight_ref, put):
    half = weight_ref.shape[0]
    y, z = where_ref[0], where_ref[1]
    piece = half // 8
    for row in range(4):
        rows = []
        for residue in range(2):
            at = lax.rem(row + 4 - y, 4) * 2 + lax.rem(residue + z, 2)
            rows.append(weight_ref[pl.ds(pl.multiple_of(at * piece, piece), piece), :])
        put(row * 2 * piece, nt(grads, jnp.concatenate(rows, axis=0)).astype(BF))


def far_kernel(where_ref, grad_ref, weight_ref, out_ref):
    def put(column, value):
        out_ref[:, column : column + value.shape[1]] = value

    half_product(where_ref, grad_ref[...], weight_ref, put)


def far(where, key_grad, weight):
    tokens, keys = key_grad.shape
    half = weight.shape[0]
    vmem = pl.BlockSpec(memory_space=VMEM)
    return pl.pallas_call(
        far_kernel,
        out_shape=jax.ShapeDtypeStruct((tokens, half), BF),
        in_specs=[pl.BlockSpec(memory_space=SMEM), vmem, vmem],
        out_specs=vmem,
        compiler_params=pltpu.CompilerParams(vmem_limit_bytes=16 << 20),
        cost_estimate=pl.CostEstimate(
            flops=2 * tokens * half * keys, bytes_accessed=2 << 20, transcendentals=0
        ),
        name="far",
    )(where, key_grad, weight)


def finish_kernel(
    my_ref, where_ref, grad_ref, near_ref, other_ref, p1, p3, begun_ref, out_ref, side, held, load_sems, sems
):
    width = p1.shape[1]
    half = near_ref.shape[1]
    core = where_ref[2]

    def column(j):
        return lax.rem(my_ref[0] + 4 - j, 4) * width

    def target(at, size):
        return out_ref.at[:, pl.ds(pl.multiple_of(at, size), size)]

    loads = [pltpu.make_async_copy(ref, held.at[i], load_sems.at[i]) for i, ref in enumerate((p1, p3))]
    for load in loads:
        load.start()
    stores = [pltpu.make_async_copy(near_ref, target(column(2) + core * half, half), sems.at[0])]
    stores[0].start()

    def put(at, value):
        side[:, at : at + value.shape[1]] = value

    half_product(where_ref, grad_ref[...], other_ref, put)
    stores.append(pltpu.make_async_copy(side, target(column(2) + (1 - core) * half, half), sems.at[1]))
    stores[1].start()
    for i, j in enumerate((1, 3)):
        loads[i].wait()
        store = pltpu.make_async_copy(held.at[i], target(column(j), width), sems.at[2 + i])
        store.start()
        stores.append(store)
    for store in stores:
        store.wait()


def finish(my, where, key_grad, near, other, p1, p3, begun):
    tokens, width = p1.shape
    vmem = pl.BlockSpec(memory_space=VMEM)
    smem = pl.BlockSpec(memory_space=SMEM)
    hbm = pl.BlockSpec(memory_space=pltpu.HBM)
    return pl.pallas_call(
        finish_kernel,
        out_shape=jax.ShapeDtypeStruct((tokens, 4 * width), BF),
        in_specs=[smem, smem, vmem, vmem, vmem, hbm, hbm, hbm],
        out_specs=hbm,
        input_output_aliases={7: 0},
        scratch_shapes=[
            VMEM((tokens, other.shape[0]), BF),
            VMEM((2, tokens, width), BF),
            pltpu.SemaphoreType.DMA((2,)),
            pltpu.SemaphoreType.DMA((4,)),
        ],
        compiler_params=pltpu.CompilerParams(vmem_limit_bytes=FINISH_LIMIT << 20),
        cost_estimate=pl.CostEstimate(flops=200_000_000, bytes_accessed=6 << 20, transcendentals=0),
        name="finish",
    )(my, where, key_grad, near, other, p1, p3, begun)


def shift(x, k, n=4):
    return lax.ppermute(x, "shard", [(i, (i + k) % n) for i in range(n)])


def after(x, *earlier):
    return lax.optimization_barrier((x, *earlier))[0]


def turn(x, dy, dz, dc):
    pairs = []
    for y in range(4):
        for z in range(8):
            for c in range(2):
                to = (((y + dy) % 4) * 8 + (z ^ dz)) * 2 + (c ^ dc)
                pairs.append(((y * 8 + z) * 2 + c, to))
    return lax.ppermute(x, "rep", pairs)


def step(activ, key_grad, key_weight, feedback, kept, region_len):
    shards = lax.axis_size("shard")
    my = lax.axis_index("shard")
    rep = lax.axis_index("rep")
    me = rep.reshape(1)
    my1 = my.reshape(1)
    y, z, core = lax.div(rep, 16), lax.rem(lax.div(rep, 2), 8), lax.rem(rep, 2)
    where = jnp.stack([y, z, core])
    owners = lax.axis_size("rep")
    width = activ.shape[1] // shards
    piece = width // 16
    index = ((core * 4 + y) * 2 + lax.rem(z, 2)).reshape(1)
    grad_one = shift(key_grad, 1)
    grad_three = shift(key_grad, 3)
    one, three, mine = pack(my1, index, activ, key_weight, width, piece)
    mine = shift(mine, 2)
    bundle, back = {}, {}
    bundle[1] = shift(one, 1)
    bundle[3] = shift(three, 3)
    twin = turn(mine, 0, 1, 0)
    table = feedback[0]
    blocks = table.shape[0]
    mean_len = blocks // owners
    send, two = prep(me, my1, kept, region_len, table, activ, key_grad, owners)
    bundle[2] = shift(two, 2)
    plane = join([mine, twin])
    grid = [plane, None, None, None]
    for dy in (1, 3, 2):
        grid[dy] = turn(plane, -dy, 0, 0)
    got = lax.all_to_all(send, "rep", split_axis=0, concat_axis=0, tiled=True)
    begun, *parts = dots(my1, key_grad, [grad_one, grad_three], key_weight)
    for k, part in zip((1, 3), parts):
        back[k] = shift(part, shards - k)
    near = join(grid)
    other = turn(near, 0, 0, 1)
    near_part = far(where, key_grad, near)
    updated = grad_update(my1, activ, key_grad, [bundle[1], bundle[2], bundle[3]], [grad_one, grad_three], table, kept)
    last = after(back[1], updated)
    input_grad = finish(my1, where, key_grad, near_part, other, back[3], last, begun)
    owned_rows = owned(got, mean_len + mean_len // 2)
    return (input_grad, updated[None], owned_rows[None])


def solution(mesh):
    return jax.shard_map(
        step,
        mesh=mesh,
        in_specs=(
            P(("rep", "shard"), None),
            P(("rep", "shard"), None),
            P("shard", None),
            P("rep", "shard", None),
            P("rep", "shard", None),
            P("shard", None),
        ),
        out_specs=(P(("rep", "shard"), None), P("rep", "shard", None), P("shard", "rep", None)),
        check_vma=False,
    )
```
